32 devices in a mesh: seq: 8 (over z, x), head: 4 (over y, core).
Axes of the slice: x: 2, y: 2, z: 4, core: 2. Of those that a mesh axis runs over, the one named last changes fastest.
Arguments:
- tokens: bfloat16 [2048, 3584], P('seq'), may hold values from -16 to 16
- length: int32 [1], replicated, may hold values from 512 to 2048
- in_gain: float32 [3584], replicated, may hold values from 0.5 to 1.5
- q_weight: bfloat16 [3584, 3584], P(None, 'head'), may hold values from -0.09375 to 0.09375
- q_bias: float32 [3584], P('head'), may hold values from -60 to 60
- k_weight: bfloat16 [3584, 512], P(None, 'head'), may hold values from -0.09375 to 0.09375
- k_bias: float32 [512], P('head'), may hold values from -60 to 60
- v_weight: bfloat16 [3584, 512], P(None, 'head'), may hold values from -0.09375 to 0.09375
- v_bias: float32 [512], P('head'), may hold values from -2 to 2
- o_weight: bfloat16 [3584, 3584], P('head'), may hold values from -0.125 to 0.125
- final_gain: float32 [3584], P('head'), may hold values from 0.5 to 1.5
Outputs:
- hidden: bfloat16 [2048, 3584], P('seq', 'head')
- embedding: float32 [3584], P('head')
The draws below stay inside these ranges and needn't reach their ends.
All inputs are finite; a program needn't handle non-finite values.
Results may differ from the reference program's by a relative error of at most 0.0075.
The reference program's roundings to bfloat16 on the way (of `normed`, `query` and `attended`) count: a program that leaves them out, or rounds other values in their place, can miss the bound.
Values may be sent and summed in bfloat16 or wider, within the bound.
A program may use at most 192 MiB of HBM per device.

```python
import jax
import jax.numpy as jnp
from jax import lax

D = 3584
HEADS = 28
KV_HEADS = 4
HEAD_DIM = 128
TOKENS = 2048


def draw_tokens(key, part):
    place = (jnp.arange(D, dtype=jnp.float32) + 0.5) / D
    tilt = jax.random.uniform(jax.random.fold_in(key, 11), (TOKENS, 1), jnp.float32, -1.0, 1.0)
    noise = jnp.clip(jax.random.normal(jax.random.fold_in(key, 12), (TOKENS, D), jnp.float32), -6.0, 6.0)
    scale = jnp.exp(tilt * 0.92 * (2.0 * place[None, :] - 1.0))
    return (noise * scale).astype(jnp.bfloat16)


def draw_k_bias(key, part):
    noise = 0.3 * jnp.clip(jax.random.normal(jax.random.fold_in(key, 1), (KV_HEADS * HEAD_DIM,), jnp.float32), -6.0, 6.0)
    return noise


def draw_q_bias(key, part):
    noise = 0.3 * jnp.clip(jax.random.normal(jax.random.fold_in(key, 2), (HEADS * HEAD_DIM,), jnp.float32), -6.0, 6.0)
    return noise


def with_spikes(array, own_key, source, target, blocks, factor):
    owner, partner = [(jnp.arange(array.shape[dim]) // (array.shape[dim] // blocks)).reshape([-1 if axis == dim else 1 for axis in range(array.ndim)]) for dim in (source, target)]
    chosen = jax.random.permutation(own_key, blocks)[partner]
    strong = (owner == chosen) | (owner == (partner + blocks // 2) % blocks)
    return jnp.where(strong, factor * array, array)


def block_levels(stream_key, extent, split, least, high):
    loudness = 1.0
    for axis_at, blocks in split:
        heights = jax.random.uniform(jax.random.fold_in(jax.random.fold_in(stream_key, 6), axis_at), (blocks,), jnp.float32, least / len(split), high / len(split))
        loudness = loudness * jnp.repeat(jnp.exp(heights), extent[axis_at] // blocks).reshape((-1,) + (1,) * (len(extent) - 1 - axis_at))
    return loudness


def bell_draw(own_key, shape, deviation, limit, pieces=(), held_as=jnp.bfloat16):
    loudness = block_levels(own_key, shape, pieces, -0.22, 0.18) if pieces else 1.0
    entries = jax.random.normal(own_key, shape, jnp.float32) * deviation * loudness
    return jnp.minimum(jnp.maximum(entries, -limit), limit).astype(held_as)


def bell_draw_with(own_key, dims, spread, most, split, heavy, held_as=jnp.bfloat16):
    entries = spread * jax.random.normal(own_key, dims, jnp.float32)
    if split:
        entries = entries * block_levels(own_key, dims, split, -0.22, 0.18)
    return jnp.clip(with_spikes(entries, jax.random.fold_in(own_key, 3), *heavy), -most, most).astype(held_as)


def setup_inputs(seed: int = 0) -> dict:
    key_of = jax.random.split(jax.random.key(seed), 12)
    return {
        "tokens": draw_tokens(jax.random.fold_in(key_of[11], 71), 0),
        "length": jax.random.randint(key_of[1], (1,), TOKENS // 4, TOKENS + 1).astype(jnp.int32),
        "in_gain": jnp.clip(1.0 + 0.1 * jax.random.normal(key_of[2], (D,), jnp.float32), 0.5, 1.5),
        "q_weight": bell_draw(key_of[3], (D, HEADS * HEAD_DIM), D ** -0.5, 0.09375, ((1, 4),)),
        "q_bias": draw_q_bias(jax.random.fold_in(key_of[11], 71), 0),
        "k_weight": bell_draw(key_of[5], (D, KV_HEADS * HEAD_DIM), D ** -0.5, 0.09375, ((1, 4),)),
        "k_bias": draw_k_bias(jax.random.fold_in(key_of[11], 71), 0),
        "v_weight": bell_draw(key_of[7], (D, KV_HEADS * HEAD_DIM), D ** -0.5, 0.09375, ((1, 4),)),
        "v_bias": bell_draw(key_of[8], (KV_HEADS * HEAD_DIM,), 0.3, 2.0, ((0, 4),), jnp.float32),
        "o_weight": bell_draw_with(key_of[9], (HEADS * HEAD_DIM, D), (HEADS * HEAD_DIM) ** -0.5, 0.125, ((0, 4),), (0, 1, 4, 2.0)),
        "final_gain": jnp.clip(1.0 + 0.1 * jax.random.normal(key_of[10], (D,), jnp.float32), 0.5, 1.5),
    }


rope_base = 1000000.0
epsilon = 1e-06

def rms_norm(inputs, gain):
    inputs = inputs.astype(jnp.float32)
    return inputs * lax.rsqrt(lax.optimization_barrier(jnp.mean(inputs * inputs, axis=-1, keepdims=True)) + epsilon) * gain

def rope_tables(positions):
    half_dim = HEAD_DIM // 2
    inverse = rope_base ** (-(jnp.arange(half_dim, dtype=jnp.float32) * 2.0) / HEAD_DIM)
    angles = positions.astype(jnp.float32)[:, None] * inverse[None, :]
    angles = jnp.concatenate([angles, angles], axis=1)
    return (jnp.cos(angles), jnp.sin(angles))

def rotate(inputs, cosine, sine):
    half_dim = HEAD_DIM // 2
    turned = jnp.concatenate([-inputs[..., half_dim:], inputs[..., :half_dim]], axis=-1)
    return inputs * cosine[:, None, :] + turned * sine[:, None, :]

def reference(tokens, length, in_gain, q_weight, q_bias, k_weight, k_bias, v_weight, v_bias, o_weight, final_gain):
    seq_len = tokens.shape[0]
    group_size = HEADS // KV_HEADS
    normed = rms_norm(tokens, in_gain).astype(jnp.bfloat16)
    cosine, sine = rope_tables(jnp.arange(seq_len, dtype=jnp.int32))
    query = jnp.dot(normed, q_weight, preferred_element_type=jnp.float32) + q_bias
    query = (rotate(query.reshape(seq_len, HEADS, HEAD_DIM), cosine, sine) * HEAD_DIM ** (-0.5)).astype(jnp.bfloat16)
    keys = jnp.dot(normed, k_weight, preferred_element_type=jnp.float32) + k_bias
    keys = rotate(keys.reshape(seq_len, KV_HEADS, HEAD_DIM), cosine, sine).astype(jnp.bfloat16)
    values = (jnp.dot(normed, v_weight, preferred_element_type=jnp.float32) + v_bias).astype(jnp.bfloat16)
    values = values.reshape(seq_len, KV_HEADS, HEAD_DIM)
    live = jnp.arange(seq_len, dtype=jnp.int32) < length[0]

    def one_head(index):
        kv_index = index // group_size
        q_head = lax.dynamic_index_in_dim(query, index, 1, keepdims=False)
        k_head = lax.dynamic_index_in_dim(keys, kv_index, 1, keepdims=False)
        v_head = lax.dynamic_index_in_dim(values, kv_index, 1, keepdims=False)
        scores = lax.dot_general(q_head, k_head, (((1,), (1,)), ((), ())), preferred_element_type=jnp.float32)
        scores = jnp.where(live[None, :], scores, -1e+30)
        top = lax.optimization_barrier(jnp.max(scores, axis=1, keepdims=True))
        weights = jnp.where(live[None, :], jnp.exp(scores - top), 0.0)
        total = lax.optimization_barrier(jnp.sum(weights, axis=1, keepdims=True))
        mixed = jnp.dot(weights.astype(jnp.bfloat16), v_head, preferred_element_type=jnp.float32)
        return (mixed / total).astype(jnp.bfloat16)
    heads_out = lax.map(one_head, jnp.arange(HEADS, dtype=jnp.int32))
    attended = jnp.transpose(heads_out, (1, 0, 2)).reshape(seq_len, HEADS * HEAD_DIM)
    hidden_full = tokens.astype(jnp.float32) + jnp.dot(attended, o_weight, preferred_element_type=jnp.float32)
    hidden = hidden_full.astype(jnp.bfloat16)
    final = rms_norm(hidden_full, final_gain)
    pooled_sum = lax.optimization_barrier(jnp.sum(jnp.where(live[:, None], final, 0.0), axis=0))
    mean = pooled_sum / length[0].astype(jnp.float32)
    embedding = mean * lax.rsqrt(jnp.mean(mean * mean) + epsilon)
    return (hidden, embedding)
```

```python
import functools

import jax
import jax.numpy as jnp
import numpy as np
from jax import lax
from jax.experimental import pallas as pl
from jax.experimental.pallas import tpu as pltpu
from jax.sharding import PartitionSpec as P

HEAD_DIM = 128
ROPE_BASE = 1000000.0
EPS = 1e-06
MESH = pl.DeviceIdType.MESH
F32 = jnp.float32
BF16 = jnp.bfloat16
LOW = -1e30


def widths(share):
    out, at = [], 0
    first = share % 256 or 256
    while at < share:
        width = first if at == 0 else 256
        out.append((at, width))
        at += width
    return out


def dot(a, b):
    return jnp.dot(a, b, preferred_element_type=F32)


def kernel(
    n_seq,
    n_head,
    length_ref,
    tokens_hbm,
    gain_ref,
    wq_hbm,
    qb_ref,
    wk_hbm,
    kb_ref,
    wv_hbm,
    vb_ref,
    wo_hbm,
    fgain_ref,
    cos_row,
    sin_row,
    cos_off,
    sin_off,
    hidden_hbm,
    emb_ref,
    tok,
    normed,
    wkv,
    wq,
    wo,
    cos,
    sin,
    qt,
    kbuf,
    vbuf,
    m_ref,
    l_ref,
    acc_ref,
    att,
    hid,
    hid_bf,
    sqbuf,
    pbuf,
    wbuf,
    local_sem,
    ring_send,
    ring_recv,
    pair_send,
    pair_recv,
    cross_send,
    cross_recv,
    sq_send,
    sq_recv,
    pool_send,
    pool_recv,
    pow_send,
    pow_recv,
    *chunk_bufs,
):
    rows, width = tok.shape
    share = hid.shape[1]
    heads = qt.shape[0]
    half = n_seq // 2
    n_y = n_head // 2
    chunks = widths(share)
    psend, precv = chunk_bufs[0::5], chunk_bufs[1::5]
    pown, ysend, yrecv = chunk_bufs[2::5], chunk_bufs[3::5], chunk_bufs[4::5]
    ms = lax.axis_index("seq")
    mh = lax.axis_index("head")
    limit = length_ref[0]

    loads = [
        pltpu.make_async_copy(tokens_hbm, tok, local_sem.at[0]),
        pltpu.make_async_copy(wk_hbm, wkv.at[:, :HEAD_DIM], local_sem.at[1]),
        pltpu.make_async_copy(wv_hbm, wkv.at[:, HEAD_DIM:], local_sem.at[2]),
        pltpu.make_async_copy(wq_hbm, wq, local_sem.at[3]),
        pltpu.make_async_copy(wo_hbm, wo, local_sem.at[4]),
    ]
    for load in loads:
        load.start()

    barrier = pltpu.get_barrier_semaphore()

    def greet(d, carry):
        pl.semaphore_signal(
            barrier, inc=1, device_id={"seq": lax.rem(ms + d, n_seq)}, device_id_type=MESH
        )
        return carry

    lax.fori_loop(1, n_seq, greet, 0)
    for d in range(1, n_head):
        pl.semaphore_signal(
            barrier, inc=1, device_id={"head": lax.rem(mh + d, n_head)}, device_id_type=MESH
        )

    far = pl.ds(pl.multiple_of(ms * 8, 8), 8)
    co, so = cos_off[far, :][:1], sin_off[far, :][:1]
    lane = lax.broadcasted_iota(jnp.int32, (1, HEAD_DIM), 1)
    sign = jnp.where(lane < HEAD_DIM // 2, -1.0, 1.0)
    cos[...] = cos_row[...] * co - sin_row[...] * so
    sin[...] = (sin_row[...] * co + cos_row[...] * so) * sign

    def rope(u):
        return u * cos[...] + pltpu.roll(u, HEAD_DIM // 2, 1) * sin[...]

    loads[0].wait()
    block = 16

    def norm_block(i, carry):
        at = pl.ds(pl.multiple_of(i * block, block), block)
        x = tok[at, :].astype(F32)
        mean = jnp.sum(x * x, axis=1, keepdims=True) / width
        normed[at, :] = (x * lax.rsqrt(mean + EPS) * gain_ref[...]).astype(BF16)
        return carry

    lax.fori_loop(0, rows // block, norm_block, 0)

    loads[1].wait()
    loads[2].wait()
    kv = dot(normed[...], wkv[...])
    kbuf[ms] = rope(kv[:, :HEAD_DIM] + kb_ref[...]).astype(BF16)
    vbuf[ms] = jnp.transpose(kv[:, HEAD_DIM:] + vb_ref[...]).astype(BF16)

    q2 = lax.div(ms, 2)
    pos = q2 + (ms - 2 * q2) * (n_seq - 1 - 2 * q2)

    def slot(p):
        p = lax.rem(p + 2 * n_seq, n_seq)
        back = lax.div(p, half)
        return (1 - back) * 2 * p + back * (2 * (n_seq - 1 - p) + 1)

    ends = (slot(pos + 1), slot(pos - 1))

    def moved(way, kind, s, hops):
        sign_of = 1 if way == 0 else -1
        at = slot(pos - sign_of * hops)
        buf = vbuf if kind else kbuf
        return pltpu.make_async_remote_copy(
            src_ref=buf.at[at],
            dst_ref=buf.at[at],
            send_sem=ring_send.at[2 * way + kind, s],
            recv_sem=ring_recv.at[2 * way + kind, s],
            device_id={"seq": ends[way]},
            device_id_type=MESH,
        )

    def send(way, kind, s):
        return moved(way, kind, s, s - 1)

    def arrival(way, kind, s):
        return moved(way, kind, s, s)

    pl.semaphore_wait(barrier, n_seq + n_head - 2)
    for kind in (0, 1):
        for way in (0, 1):
            send(way, kind, 1).start()

    def put_query(h, u):
        at = pl.ds(pl.multiple_of(h * HEAD_DIM, HEAD_DIM), HEAD_DIM)
        u = rope(u + qb_ref[:, at]) * HEAD_DIM ** (-0.5)
        qt[h] = jnp.transpose(u).astype(BF16)

    loads[3].wait()

    def query_pair(j, carry):
        at = pl.ds(pl.multiple_of(j * 2 * HEAD_DIM, 2 * HEAD_DIM), 2 * HEAD_DIM)
        u = dot(normed[...], wq[:, at])
        put_query(2 * j, u[:, :HEAD_DIM])
        put_query(2 * j + 1, u[:, HEAD_DIM:])
        return carry

    lax.fori_loop(0, heads // 2, query_pair, 0)
    if heads % 2:
        put_query(heads - 1, dot(normed[...], wq[:, (heads - 1) * HEAD_DIM :]))

    def attend(blocks, first):
        def per_head(h, carry):
            query = qt[h]
            scores = []
            for b in blocks:
                s = dot(kbuf[b], query)
                key_at = b * rows + lax.broadcasted_iota(jnp.int32, (rows, 1), 0)
                scores.append(jnp.where(key_at < limit, s, LOW))
            tops = [jnp.max(s, axis=0, keepdims=True) for s in scores]
            top = functools.reduce(jnp.maximum, tops)
            if not first:
                old = m_ref[h][:1]
                top = jnp.maximum(old, top)
                alpha = jnp.exp(old - top)
            total, mixed = None, None
            for b, s in zip(blocks, scores):
                p = jnp.exp(s - top)
                part = jnp.sum(p, axis=0, keepdims=True)
                prod = dot(vbuf[b], p.astype(BF16))
                total = part if total is None else total + part
                mixed = prod if mixed is None else mixed + prod
            if not first:
                total = total + l_ref[h][:1] * alpha
                mixed = mixed + acc_ref[h] * alpha
            m_ref[h] = jnp.broadcast_to(top, (8, rows))
            l_ref[h] = jnp.broadcast_to(total, (8, rows))
            acc_ref[h] = mixed
            return carry

        lax.fori_loop(0, heads, per_head, 0)

    def forward(s, kinds_ways):
        for kind in (0, 1):
            for way in (0, 1):
                arrival(way, kind, s).wait_recv()
                if (way, kind) in kinds_ways:
                    send(way, kind, s + 1).start()

    every = ((0, 0), (0, 1), (1, 0), (1, 1))
    last = ((0, 0), (1, 1))
    forward(1, every if half > 2 else last)
    attend([ms], True)
    attend([slot(pos - 1), slot(pos + 1)], False)

    def ring_step(s, carry):
        forward(s, every)
        attend([slot(pos - s), slot(pos + s)], False)
        return carry

    if half > 3:
        lax.fori_loop(2, half - 1, ring_step, 0)
    if half > 2:
        forward(half - 1, last)
        attend([slot(pos - half + 1), slot(pos + half - 1)], False)
    for way, kind in last:
        arrival(way, kind, half).wait_recv()
    attend([slot(pos - half)], False)

    def finish(h, carry):
        at = pl.ds(pl.multiple_of(h * HEAD_DIM, HEAD_DIM), HEAD_DIM)
        att[:, at] = jnp.transpose(acc_ref[h] / l_ref[h][:1]).astype(BF16)
        return carry

    lax.fori_loop(0, heads, finish, 0)

    loads[4].wait()
    my = lax.div(mh, 2)
    mc = mh - 2 * my
    partner = 2 * my + 1 - mc

    def partial(dest, at, wide):
        cols = pl.ds(pl.multiple_of(dest * share + at, HEAD_DIM), wide)
        return dot(att[...], wo[:, cols])

    def pair_copy(i):
        return pltpu.make_async_remote_copy(
            src_ref=psend[i],
            dst_ref=precv[i],
            send_sem=pair_send.at[i],
            recv_sem=pair_recv.at[i],
            device_id={"head": partner},
            device_id_type=MESH,
        )

    def cross_copy(i, d):
        return pltpu.make_async_remote_copy(
            src_ref=ysend[i].at[d - 1],
            dst_ref=yrecv[i].at[d - 1],
            send_sem=cross_send.at[i, d - 1],
            recv_sem=cross_recv.at[i, d - 1],
            device_id={"head": 2 * lax.rem(my + d, n_y) + mc},
            device_id_type=MESH,
        )

    def to_partner(i):
        at, wide = chunks[i]
        for y in range(n_y):
            psend[i][y] = partial(2 * y + 1 - mc, at, wide).astype(BF16)
        pair_copy(i).start()
        for d in range(1, n_y):
            pown[i][d] = partial(2 * lax.rem(my + d, n_y) + mc, at, wide)

    def across(i):
        pair_copy(i).wait_recv()
        for d in range(1, n_y):
            y = lax.rem(my + d, n_y)
            ysend[i][d - 1] = (pown[i][d] + precv[i][y].astype(F32)).astype(BF16)
            cross_copy(i, d).start()

    for i in range(len(chunks)):
        to_partner(i)
        if i:
            across(i - 1)
    across(len(chunks) - 1)
    for i, (at, wide) in enumerate(chunks):
        pown[i][0] = partial(mh, at, wide)

    squares = None
    outs = []
    for i, (at, wide) in enumerate(chunks):
        mine = pl.ds(pl.multiple_of(mh * share + at, HEAD_DIM), wide)
        base = tok[:, mine].astype(F32) + (pown[i][0] + precv[i][my].astype(F32))
        for d in range(1, n_y):
            cross_copy(i, d).wait_recv()
            base = base + yrecv[i][d - 1].astype(F32)
        hid[:, at : at + wide] = base
        hid_bf[:, at : at + wide] = base.astype(BF16)
        for g in range(0, wide, HEAD_DIM):
            piece = base[:, g : g + HEAD_DIM]
            squares = piece * piece if squares is None else squares + piece * piece
    out_copy = pltpu.make_async_copy(hid_bf, hidden_hbm, local_sem.at[5])
    out_copy.start()

    def head_copy(buf, send_sems, recv_sems, d):
        return pltpu.make_async_remote_copy(
            src_ref=buf.at[mh],
            dst_ref=buf.at[mh],
            send_sem=send_sems.at[d - 1],
            recv_sem=recv_sems.at[d - 1],
            device_id={"head": lax.rem(mh + d, n_head)},
            device_id_type=MESH,
        )

    def head_arrival(buf, send_sems, recv_sems, d):
        source = lax.rem(mh + n_head - d, n_head)
        return pltpu.make_async_remote_copy(
            src_ref=buf.at[source],
            dst_ref=buf.at[source],
            send_sem=send_sems.at[d - 1],
            recv_sem=recv_sems.at[d - 1],
            device_id={"head": source},
            device_id_type=MESH,
        )

    def head_sum(buf, send_sems, recv_sems, value):
        buf[mh] = jnp.broadcast_to(value, buf.shape[1:])
        for d in range(1, n_head):
            head_copy(buf, send_sems, recv_sems, d).start()
        for d in range(1, n_head):
            head_arrival(buf, send_sems, recv_sems, d).wait_recv()
        return functools.reduce(lambda a, b: a + b, [buf[d][:1] for d in range(n_head)])

    square_row = jnp.sum(jnp.transpose(squares), axis=0, keepdims=True)
    power = head_sum(sqbuf, sq_send, sq_recv, square_row)
    place = ms * rows + lax.broadcasted_iota(jnp.int32, (1, rows), 1)
    scale = jnp.where(place < limit, lax.rsqrt(power / width + EPS), 0.0)
    scale = jnp.transpose(jnp.broadcast_to(scale, (HEAD_DIM, rows)))

    groups = pbuf.shape[1]
    sums = []
    for g in range(0, share, HEAD_DIM):
        at = slice(g, g + HEAD_DIM)
        sums.append(jnp.sum(hid[:, at] * scale, axis=0, keepdims=True) * fgain_ref[:, at])
    sums += [jnp.zeros((1, HEAD_DIM), F32)] * (groups - len(sums))
    pbuf[ms] = jnp.concatenate(sums, axis=0)

    def pool_copy(d):
        return pltpu.make_async_remote_copy(
            src_ref=pbuf.at[ms],
            dst_ref=pbuf.at[ms],
            send_sem=pool_send.at[d - 1],
            recv_sem=pool_recv.at[d - 1],
            device_id={"seq": lax.rem(ms + d, n_seq)},
            device_id_type=MESH,
        )

    def pool_start(d, carry):
        pool_copy(d).start()
        return carry

    def pool_wait(d, carry):
        source = lax.rem(ms + n_seq - d, n_seq)
        pltpu.make_async_remote_copy(
            src_ref=pbuf.at[source],
            dst_ref=pbuf.at[source],
            send_sem=pool_send.at[d - 1],
            recv_sem=pool_recv.at[d - 1],
            device_id={"seq": source},
            device_id_type=MESH,
        ).wait_recv()
        return carry

    lax.fori_loop(1, n_seq, pool_start, 0)
    lax.fori_loop(1, n_seq, pool_wait, 0)
    mean = functools.reduce(lambda a, b: a + b, [pbuf[d] for d in range(n_seq)])
    mean = mean / limit.astype(F32)
    total = head_sum(wbuf, pow_send, pow_recv, jnp.sum(mean * mean, axis=0, keepdims=True))
    pooled = mean * lax.rsqrt(jnp.sum(total, axis=1, keepdims=True) / width + EPS)
    for g in range(share // HEAD_DIM):
        emb_ref[:, g * HEAD_DIM : (g + 1) * HEAD_DIM] = pooled[g : g + 1]

    def sent(s, carry):
        for way, kind in every:
            send(way, kind, s).wait_send()
        return carry

    lax.fori_loop(1, half, sent, 0)
    for way, kind in last:
        send(way, kind, half).wait_send()
    for i in range(len(chunks)):
        pair_copy(i).wait_send()
        for d in range(1, n_y):
            cross_copy(i, d).wait_send()
    for d in range(1, n_head):
        head_copy(sqbuf, sq_send, sq_recv, d).wait_send()
        head_copy(wbuf, pow_send, pow_recv, d).wait_send()

    def pool_sent(d, carry):
        pool_copy(d).wait_send()
        return carry

    lax.fori_loop(1, n_seq, pool_sent, 0)
    out_copy.wait()


def body(
    n_seq,
    n_head,
    tokens,
    length,
    in_gain,
    q_weight,
    q_bias,
    k_weight,
    k_bias,
    v_weight,
    v_bias,
    o_weight,
    final_gain,
):
    rows, width = tokens.shape
    share = width // n_head
    heads = q_weight.shape[1] // HEAD_DIM
    half = n_seq // 2
    n_y = n_head // 2
    inverse = ROPE_BASE ** (-(np.arange(HEAD_DIM // 2) * 2.0) / HEAD_DIM)
    inverse = np.concatenate([inverse, inverse])[None, :]
    near = np.arange(rows)[:, None] * inverse
    far = np.repeat(np.arange(n_seq) * rows, 8)[:, None] * inverse
    tables = [f(a).astype(np.float32) for a in (near, far) for f in (np.cos, np.sin)]

    chunks = widths(share)
    groups = -(-share // (8 * HEAD_DIM)) * 8
    chunk_bufs = []
    for _, wide in chunks:
        chunk_bufs += [
            pltpu.VMEM((n_y, rows, wide), BF16),
            pltpu.VMEM((n_y, rows, wide), BF16),
            pltpu.VMEM((n_y, rows, wide), F32),
            pltpu.VMEM((n_y - 1, rows, wide), BF16),
            pltpu.VMEM((n_y - 1, rows, wide), BF16),
        ]
    dma = pltpu.SemaphoreType.DMA
    hbm = pl.BlockSpec(memory_space=pl.ANY)
    vmem = pl.BlockSpec(memory_space=pltpu.VMEM)
    smem = pl.BlockSpec(memory_space=pltpu.SMEM)
    hidden, embedding = pl.pallas_call(
        functools.partial(kernel, n_seq, n_head),
        out_shape=(
            jax.ShapeDtypeStruct((rows, share), BF16),
            jax.ShapeDtypeStruct((1, share), F32),
        ),
        in_specs=[smem, hbm, vmem, hbm, vmem, hbm, vmem, hbm, vmem, hbm] + [vmem] * 5,
        out_specs=(hbm, vmem),
        scratch_shapes=[
            pltpu.VMEM((rows, width), BF16),
            pltpu.VMEM((rows, width), BF16),
            pltpu.VMEM((width, 2 * HEAD_DIM), BF16),
            pltpu.VMEM(q_weight.shape, BF16),
            pltpu.VMEM(o_weight.shape, BF16),
            pltpu.VMEM((rows, HEAD_DIM), F32),
            pltpu.VMEM((rows, HEAD_DIM), F32),
            pltpu.VMEM((heads, HEAD_DIM, rows), BF16),
            pltpu.VMEM((n_seq, rows, HEAD_DIM), BF16),
            pltpu.VMEM((n_seq, HEAD_DIM, rows), BF16),
            pltpu.VMEM((heads, 8, rows), F32),
            pltpu.VMEM((heads, 8, rows), F32),
            pltpu.VMEM((heads, HEAD_DIM, rows), F32),
            pltpu.VMEM((rows, heads * HEAD_DIM), BF16),
            pltpu.VMEM((rows, share), F32),
            pltpu.VMEM((rows, share), BF16),
            pltpu.VMEM((n_head, 8, rows), F32),
            pltpu.VMEM((n_seq, groups, HEAD_DIM), F32),
            pltpu.VMEM((n_head, 8, HEAD_DIM), F32),
            dma((6,)),
            dma((4, half + 1)),
            dma((4, half + 1)),
            dma((len(chunks),)),
            dma((len(chunks),)),
            dma((len(chunks), n_y)),
            dma((len(chunks), n_y)),
            dma((n_head,)),
            dma((n_head,)),
            dma((n_seq,)),
            dma((n_seq,)),
            dma((n_head,)),
            dma((n_head,)),
        ]
        + chunk_bufs,
        compiler_params=pltpu.CompilerParams(
            collective_id=0, has_side_effects=True, vmem_limit_bytes=60 * 1024 * 1024
        ),
    )(
        length,
        tokens,
        in_gain[None, :],
        q_weight,
        q_bias[None, :],
        k_weight,
        k_bias[None, :],
        v_weight,
        v_bias[None, :],
        o_weight,
        final_gain[None, :],
        *tables,
    )
    return hidden, embedding[0]


def solution(mesh):
    in_specs = (
        P("seq", None),
        P(),
        P(),
        P(None, "head"),
        P("head"),
        P(None, "head"),
        P("head"),
        P(None, "head"),
        P("head"),
        P("head", None),
        P("head"),
    )
    out_specs = (P("seq", "head"), P("head"))
    step = functools.partial(body, mesh.shape["seq"], mesh.shape["head"])
    return jax.shard_map(step, mesh=mesh, in_specs=in_specs, out_specs=out_specs, check_vma=False)
```

```python
import functools

import jax
import jax.numpy as jnp
import numpy as np
from jax import lax
from jax.experimental import pallas as pl
from jax.experimental.pallas import tpu as pltpu
from jax.sharding import PartitionSpec as P

HEAD_DIM = 128
ROPE_BASE = 1000000.0
EPS = 1e-06
MESH = pl.DeviceIdType.MESH
F32 = jnp.float32
BF16 = jnp.bfloat16
LOW = -1e30


def widths(share):
    out, at = [], 0
    first = share % 256 or 256
    while at < share:
        width = first if at == 0 else 256
        out.append((1, at, width))
        at += width
    cut = out[len(out) // 2][1]
    return [(0, 0, cut), (0, cut, share - cut)] + out


def dot(a, b):
    return jnp.dot(a, b, preferred_element_type=F32)


def kernel(
    n_seq,
    n_head,
    length_ref,
    tokens_hbm,
    gain_1d,
    wq_hbm,
    qb_1d,
    wk_hbm,
    kb_1d,
    wv_hbm,
    vb_1d,
    wo_hbm,
    fgain_1d,
    cos_row,
    sin_row,
    cos_off,
    sin_off,
    hidden_hbm,
    emb_ref,
    gain_ref,
    qb_ref,
    kb_ref,
    vb_ref,
    fgain_ref,
    tok,
    normed,
    wkv,
    wq,
    wo,
    cos,
    sin,
    qt,
    kbuf,
    vbuf,
    m_ref,
    l_ref,
    acc_ref,
    att,
    hid,
    hid_bf,
    sqbuf,
    pbuf,
    wbuf,
    local_sem,
    ring_send,
    ring_recv,
    pair_send,
    pair_recv,
    cross_send,
    cross_recv,
    sq_send,
    sq_recv,
    pool_send,
    pool_recv,
    pow_send,
    pow_recv,
    *chunk_bufs,
):
    rows, width = tok.shape
    share = hid.shape[1]
    heads = qt.shape[2] // (rows // 2)
    part_rows = rows // 2
    half = n_seq // 2
    n_y = n_head // 2
    chunks = widths(share)
    psend, precv = chunk_bufs[0::5], chunk_bufs[1::5]
    pown, ysend, yrecv = chunk_bufs[2::5], chunk_bufs[3::5], chunk_bufs[4::5]
    ms = lax.axis_index("seq")
    mh = lax.axis_index("head")
    limit = length_ref[0]

    loads = [
        pltpu.make_async_copy(tokens_hbm, tok, local_sem.at[0]),
        pltpu.make_async_copy(wk_hbm, wkv.at[:, :HEAD_DIM], local_sem.at[1]),
        pltpu.make_async_copy(wv_hbm, wkv.at[:, HEAD_DIM:], local_sem.at[2]),
        pltpu.make_async_copy(wq_hbm, wq, local_sem.at[3]),
        pltpu.make_async_copy(wo_hbm, wo, local_sem.at[4]),
    ]
    for load in loads[:4]:
        load.start()

    for flat, row in (
        (gain_1d, gain_ref),
        (qb_1d, qb_ref),
        (kb_1d, kb_ref),
        (vb_1d, vb_ref),
        (fgain_1d, fgain_ref),
    ):
        for g in range(0, row.shape[1], HEAD_DIM):
            row[:, g : g + HEAD_DIM] = flat[g : g + HEAD_DIM].reshape(1, HEAD_DIM)

    barrier = pltpu.get_barrier_semaphore()

    def greet(d, carry):
        pl.semaphore_signal(
            barrier, inc=1, device_id={"seq": lax.rem(ms + d, n_seq)}, device_id_type=MESH
        )
        return carry

    lax.fori_loop(1, n_seq, greet, 0)
    for d in range(1, n_head):
        pl.semaphore_signal(
            barrier, inc=1, device_id={"head": lax.rem(mh + d, n_head)}, device_id_type=MESH
        )

    far = pl.ds(pl.multiple_of(ms * 8, 8), 8)
    co, so = cos_off[far, :][:1], sin_off[far, :][:1]
    lane = lax.broadcasted_iota(jnp.int32, (1, HEAD_DIM), 1)
    sign = jnp.where(lane < HEAD_DIM // 2, -1.0, 1.0)
    cos[...] = cos_row[...] * co - sin_row[...] * so
    sin[...] = (sin_row[...] * co + cos_row[...] * so) * sign

    def rope(u):
        return u * cos[...] + pltpu.roll(u, HEAD_DIM // 2, 1) * sin[...]

    loads[0].wait()
    block = 16

    def norm_block(i, carry):
        at = pl.ds(pl.multiple_of(i * block, block), block)
        x = tok[at, :].astype(F32)
        mean = jnp.sum(x * x, axis=1, keepdims=True) / width
        normed[at, :] = (x * lax.rsqrt(mean + EPS) * gain_ref[...]).astype(BF16)
        return carry

    lax.fori_loop(0, rows // block, norm_block, 0)

    loads[1].wait()
    loads[2].wait()
    kv = dot(normed[...], wkv[...])
    kbuf[ms] = rope(kv[:, :HEAD_DIM] + kb_ref[...]).astype(BF16)
    vbuf[ms] = jnp.transpose(kv[:, HEAD_DIM:] + vb_ref[...]).astype(BF16)

    q2 = lax.div(ms, 2)
    pos = q2 + (ms - 2 * q2) * (n_seq - 1 - 2 * q2)

    def slot(p):
        p = lax.rem(p + 2 * n_seq, n_seq)
        back = lax.div(p, half)
        return (1 - back) * 2 * p + back * (2 * (n_seq - 1 - p) + 1)

    ends = (slot(pos + 1), slot(pos - 1))

    def moved(way, kind, s, hops):
        sign_of = 1 if way == 0 else -1
        at = slot(pos - sign_of * hops)
        buf = vbuf if kind else kbuf
        return pltpu.make_async_remote_copy(
            src_ref=buf.at[at],
            dst_ref=buf.at[at],
            send_sem=ring_send.at[2 * way + kind, s],
            recv_sem=ring_recv.at[2 * way + kind, s],
            device_id={"seq": ends[way]},
            device_id_type=MESH,
        )

    def send(way, kind, s):
        return moved(way, kind, s, s - 1)

    def arrival(way, kind, s):
        return moved(way, kind, s, s)

    pl.semaphore_wait(barrier, n_seq + n_head - 2)
    for kind in (0, 1):
        for way in (0, 1):
            send(way, kind, 1).start()

    def put_query(h, u):
        at = pl.ds(pl.multiple_of(h * HEAD_DIM, HEAD_DIM), HEAD_DIM)
        to = pl.ds(pl.multiple_of(h * part_rows, part_rows), part_rows)
        u = rope(u + qb_ref[:, at]) * HEAD_DIM ** (-0.5)
        u = jnp.transpose(u).astype(BF16)
        qt[0, :, to] = u[:, :part_rows]
        qt[1, :, to] = u[:, part_rows:]

    loads[3].wait()
    loads[4].start()

    def query_pair(j, carry):
        at = pl.ds(pl.multiple_of(j * 2 * HEAD_DIM, 2 * HEAD_DIM), 2 * HEAD_DIM)
        u = dot(normed[...], wq[:, at])
        put_query(2 * j, u[:, :HEAD_DIM])
        put_query(2 * j + 1, u[:, HEAD_DIM:])
        return carry

    lax.fori_loop(0, heads // 2, query_pair, 0)
    if heads % 2:
        put_query(heads - 1, dot(normed[...], wq[:, (heads - 1) * HEAD_DIM :]))

    m_ref[...] = jnp.full(m_ref.shape, LOW, F32)
    l_ref[...] = jnp.zeros(l_ref.shape, F32)
    acc_ref[...] = jnp.zeros(acc_ref.shape, F32)
    lanes = heads * part_rows
    tiles = [(t, min(256, lanes - t)) for t in range(0, lanes, 256)]

    def attend(part, blocks):
        row_at = lax.broadcasted_iota(jnp.int32, (rows, 1), 0)
        live = [b * rows + row_at < limit for b in blocks]
        for t, wide in tiles:
            at = slice(t, t + wide)
            query = qt[part, :, at]
            scores = [jnp.where(ok, dot(kbuf[b], query), LOW) for b, ok in zip(blocks, live)]
            tops = [jnp.max(s, axis=0, keepdims=True) for s in scores]
            old = m_ref[part, :, at][:1]
            top = functools.reduce(jnp.maximum, tops, old)
            alpha = jnp.exp(old - top)
            total = l_ref[part, :, at][:1] * alpha
            mixed = acc_ref[part, :, at] * alpha
            for b, s in zip(blocks, scores):
                p = jnp.exp(s - top)
                total = total + jnp.sum(p, axis=0, keepdims=True)
                mixed = mixed + dot(vbuf[b], p.astype(BF16))
            m_ref[part, :, at] = jnp.broadcast_to(top, (8, wide))
            l_ref[part, :, at] = jnp.broadcast_to(total, (8, wide))
            acc_ref[part, :, at] = mixed

    def forward(s, kinds_ways):
        for kind in (0, 1):
            for way in (0, 1):
                arrival(way, kind, s).wait_recv()
                if (way, kind) in kinds_ways:
                    send(way, kind, s + 1).start()

    every = ((0, 0), (0, 1), (1, 0), (1, 1))
    last = ((0, 0), (1, 1))
    forward(1, every if half > 2 else last)
    attend(0, [ms])
    attend(0, [slot(pos - 1), slot(pos + 1)])

    def ring_step(s, carry):
        forward(s, every)
        attend(0, [slot(pos - s), slot(pos + s)])
        return carry

    if half > 3:
        lax.fori_loop(2, half - 1, ring_step, 0)
    if half > 2:
        forward(half - 1, last)
        attend(0, [slot(pos - half + 1), slot(pos + half - 1)])
    for way, kind in last:
        arrival(way, kind, half).wait_recv()
    attend(0, [slot(pos - half)])

    def finish(part):
        for h in range(heads):
            at = slice(h * part_rows, (h + 1) * part_rows)
            done = jnp.transpose(acc_ref[part, :, at] / l_ref[part, :, at][:1]).astype(BF16)
            cols = slice(h * HEAD_DIM, (h + 1) * HEAD_DIM)
            att[part * part_rows : (part + 1) * part_rows, cols] = done

    loads[4].wait()
    my = lax.div(mh, 2)
    mc = mh - 2 * my
    partner = 2 * my + 1 - mc

    def partial(part, dest, at, wide):
        cols = pl.ds(pl.multiple_of(dest * share + at, HEAD_DIM), wide)
        return dot(att[part * part_rows : (part + 1) * part_rows, :], wo[:, cols])

    def pair_copy(i):
        return pltpu.make_async_remote_copy(
            src_ref=psend[i],
            dst_ref=precv[i],
            send_sem=pair_send.at[i],
            recv_sem=pair_recv.at[i],
            device_id={"head": partner},
            device_id_type=MESH,
        )

    def cross_copy(i, d):
        return pltpu.make_async_remote_copy(
            src_ref=ysend[i].at[d - 1],
            dst_ref=yrecv[i].at[d - 1],
            send_sem=cross_send.at[i, d - 1],
            recv_sem=cross_recv.at[i, d - 1],
            device_id={"head": 2 * lax.rem(my + d, n_y) + mc},
            device_id_type=MESH,
        )

    def to_partner(i):
        part, at, wide = chunks[i]
        for y in range(n_y):
            psend[i][y] = partial(part, 2 * y + 1 - mc, at, wide).astype(BF16)
        pair_copy(i).start()
        for d in range(1, n_y):
            pown[i][d] = partial(part, 2 * lax.rem(my + d, n_y) + mc, at, wide)

    def across(i):
        pair_copy(i).wait_recv()
        for d in range(1, n_y):
            y = lax.rem(my + d, n_y)
            ysend[i][d - 1] = (pown[i][d] + precv[i][y].astype(F32)).astype(BF16)
            cross_copy(i, d).start()

    early = [i for i, c in enumerate(chunks) if c[0] == 0]
    late = [i for i, c in enumerate(chunks) if c[0] == 1]
    finish(0)
    for i in early:
        to_partner(i)
    attend(1, [0, 1])
    for i in early:
        across(i)

    def whole_step(i, carry):
        attend(1, [2 * i, 2 * i + 1])
        return carry

    lax.fori_loop(1, half, whole_step, 0)
    finish(1)
    for i in late:
        to_partner(i)
        if i > late[0]:
            across(i - 1)
    across(late[-1])
    for i, (part, at, wide) in enumerate(chunks):
        pown[i][0] = partial(part, mh, at, wide)

    squares = [None, None]
    for i, (part, at, wide) in enumerate(chunks):
        mine = pl.ds(pl.multiple_of(mh * share + at, HEAD_DIM), wide)
        band = slice(part * part_rows, (part + 1) * part_rows)
        base = tok[band, mine].astype(F32) + (pown[i][0] + precv[i][my].astype(F32))
        for d in range(1, n_y):
            cross_copy(i, d).wait_recv()
            base = base + yrecv[i][d - 1].astype(F32)
        hid[band, at : at + wide] = base
        hid_bf[band, at : at + wide] = base.astype(BF16)
        for g in range(0, wide, HEAD_DIM):
            piece = base[:, g : g + HEAD_DIM]
            more = piece * piece
            squares[part] = more if squares[part] is None else squares[part] + more
    squares = jnp.concatenate(squares, axis=0)
    out_copy = pltpu.make_async_copy(hid_bf, hidden_hbm, local_sem.at[5])
    out_copy.start()

    def head_copy(buf, send_sems, recv_sems, d):
        return pltpu.make_async_remote_copy(
            src_ref=buf.at[mh],
            dst_ref=buf.at[mh],
            send_sem=send_sems.at[d - 1],
            recv_sem=recv_sems.at[d - 1],
            device_id={"head": lax.rem(mh + d, n_head)},
            device_id_type=MESH,
        )

    def head_arrival(buf, send_sems, recv_sems, d):
        source = lax.rem(mh + n_head - d, n_head)
        return pltpu.make_async_remote_copy(
            src_ref=buf.at[source],
            dst_ref=buf.at[source],
            send_sem=send_sems.at[d - 1],
            recv_sem=recv_sems.at[d - 1],
            device_id={"head": source},
            device_id_type=MESH,
        )

    def head_sum(buf, send_sems, recv_sems, value):
        buf[mh] = jnp.broadcast_to(value, buf.shape[1:])
        for d in range(1, n_head):
            head_copy(buf, send_sems, recv_sems, d).start()
        for d in range(1, n_head):
            head_arrival(buf, send_sems, recv_sems, d).wait_recv()
        return functools.reduce(lambda a, b: a + b, [buf[d][:1] for d in range(n_head)])

    square_row = jnp.sum(jnp.transpose(squares), axis=0, keepdims=True)
    power = head_sum(sqbuf, sq_send, sq_recv, square_row)
    place = ms * rows + lax.broadcasted_iota(jnp.int32, (1, rows), 1)
    scale = jnp.where(place < limit, lax.rsqrt(power / width + EPS), 0.0)
    scale = jnp.transpose(jnp.broadcast_to(scale, (HEAD_DIM, rows)))

    groups = pbuf.shape[1]
    sums = []
    for g in range(0, share, HEAD_DIM):
        at = slice(g, g + HEAD_DIM)
        sums.append(jnp.sum(hid[:, at] * scale, axis=0, keepdims=True) * fgain_ref[:, at])
    sums += [jnp.zeros((1, HEAD_DIM), F32)] * (groups - len(sums))
    pbuf[ms] = jnp.concatenate(sums, axis=0)

    def pool_copy(d):
        return pltpu.make_async_remote_copy(
            src_ref=pbuf.at[ms],
            dst_ref=pbuf.at[ms],
            send_sem=pool_send.at[d - 1],
            recv_sem=pool_recv.at[d - 1],
            device_id={"seq": lax.rem(ms + d, n_seq)},
            device_id_type=MESH,
        )

    def pool_start(d, carry):
        pool_copy(d).start()
        return carry

    def pool_wait(d, carry):
        source = lax.rem(ms + n_seq - d, n_seq)
        pltpu.make_async_remote_copy(
            src_ref=pbuf.at[source],
            dst_ref=pbuf.at[source],
            send_sem=pool_send.at[d - 1],
            recv_sem=pool_recv.at[d - 1],
            device_id={"seq": source},
            device_id_type=MESH,
        ).wait_recv()
        return carry

    lax.fori_loop(1, n_seq, pool_start, 0)
    lax.fori_loop(1, n_seq, pool_wait, 0)
    mean = functools.reduce(lambda a, b: a + b, [pbuf[d] for d in range(n_seq)])
    mean = mean / limit.astype(F32)
    total = head_sum(wbuf, pow_send, pow_recv, jnp.sum(mean * mean, axis=0, keepdims=True))
    pooled = mean * lax.rsqrt(jnp.sum(total, axis=1, keepdims=True) / width + EPS)
    for g in range(share // HEAD_DIM):
        emb_ref[g * HEAD_DIM : (g + 1) * HEAD_DIM] = pooled[g : g + 1].reshape(HEAD_DIM)

    def sent(s, carry):
        for way, kind in every:
            send(way, kind, s).wait_send()
        return carry

    lax.fori_loop(1, half, sent, 0)
    for way, kind in last:
        send(way, kind, half).wait_send()
    for i in range(len(chunks)):
        pair_copy(i).wait_send()
        for d in range(1, n_y):
            cross_copy(i, d).wait_send()
    for d in range(1, n_head):
        head_copy(sqbuf, sq_send, sq_recv, d).wait_send()
        head_copy(wbuf, pow_send, pow_recv, d).wait_send()

    def pool_sent(d, carry):
        pool_copy(d).wait_send()
        return carry

    lax.fori_loop(1, n_seq, pool_sent, 0)
    out_copy.wait()


def body(
    n_seq,
    n_head,
    tokens,
    length,
    in_gain,
    q_weight,
    q_bias,
    k_weight,
    k_bias,
    v_weight,
    v_bias,
    o_weight,
    final_gain,
):
    rows, width = tokens.shape
    share = width // n_head
    heads = q_weight.shape[1] // HEAD_DIM
    half = n_seq // 2
    n_y = n_head // 2
    inverse = ROPE_BASE ** (-(np.arange(HEAD_DIM // 2) * 2.0) / HEAD_DIM)
    inverse = np.concatenate([inverse, inverse])[None, :]
    near = np.arange(rows)[:, None] * inverse
    far = np.repeat(np.arange(n_seq) * rows, 8)[:, None] * inverse
    tables = [f(a).astype(np.float32) for a in (near, far) for f in (np.cos, np.sin)]

    chunks = widths(share)
    groups = -(-share // (8 * HEAD_DIM)) * 8
    chunk_bufs = []
    for _, _, wide in chunks:
        chunk_bufs += [
            pltpu.VMEM((n_y, rows // 2, wide), BF16),
            pltpu.VMEM((n_y, rows // 2, wide), BF16),
            pltpu.VMEM((n_y, rows // 2, wide), F32),
            pltpu.VMEM((n_y - 1, rows // 2, wide), BF16),
            pltpu.VMEM((n_y - 1, rows // 2, wide), BF16),
        ]
    dma = pltpu.SemaphoreType.DMA
    hbm = pl.BlockSpec(memory_space=pl.ANY)
    vmem = pl.BlockSpec(memory_space=pltpu.VMEM)
    smem = pl.BlockSpec(memory_space=pltpu.SMEM)
    hidden, embedding = pl.pallas_call(
        functools.partial(kernel, n_seq, n_head),
        out_shape=(
            jax.ShapeDtypeStruct((rows, share), BF16),
            jax.ShapeDtypeStruct((share,), F32),
        ),
        in_specs=[smem, hbm, vmem, hbm, vmem, hbm, vmem, hbm, vmem, hbm] + [vmem] * 5,
        out_specs=(hbm, vmem),
        scratch_shapes=[
            pltpu.VMEM((1, width), F32),
            pltpu.VMEM((1, heads * HEAD_DIM), F32),
            pltpu.VMEM((1, HEAD_DIM), F32),
            pltpu.VMEM((1, HEAD_DIM), F32),
            pltpu.VMEM((1, share), F32),
            pltpu.VMEM((rows, width), BF16),
            pltpu.VMEM((rows, width), BF16),
            pltpu.VMEM((width, 2 * HEAD_DIM), BF16),
            pltpu.VMEM(q_weight.shape, BF16),
            pltpu.VMEM(o_weight.shape, BF16),
            pltpu.VMEM((rows, HEAD_DIM), F32),
            pltpu.VMEM((rows, HEAD_DIM), F32),
            pltpu.VMEM((2, HEAD_DIM, heads * (rows // 2)), BF16),
            pltpu.VMEM((n_seq, rows, HEAD_DIM), BF16),
            pltpu.VMEM((n_seq, HEAD_DIM, rows), BF16),
            pltpu.VMEM((2, 8, heads * (rows // 2)), F32),
            pltpu.VMEM((2, 8, heads * (rows // 2)), F32),
            pltpu.VMEM((2, HEAD_DIM, heads * (rows // 2)), F32),
            pltpu.VMEM((rows, heads * HEAD_DIM), BF16),
            pltpu.VMEM((rows, share), F32),
            pltpu.VMEM((rows, share), BF16),
            pltpu.VMEM((n_head, 8, rows), F32),
            pltpu.VMEM((n_seq, groups, HEAD_DIM), F32),
            pltpu.VMEM((n_head, 8, HEAD_DIM), F32),
            dma((6,)),
            dma((4, half + 1)),
            dma((4, half + 1)),
            dma((len(chunks),)),
            dma((len(chunks),)),
            dma((len(chunks), n_y)),
            dma((len(chunks), n_y)),
            dma((n_head,)),
            dma((n_head,)),
            dma((n_seq,)),
            dma((n_seq,)),
            dma((n_head,)),
            dma((n_head,)),
        ]
        + chunk_bufs,
        compiler_params=pltpu.CompilerParams(
            collective_id=0, has_side_effects=True, vmem_limit_bytes=60 * 1024 * 1024
        ),
    )(
        length,
        tokens,
        in_gain,
        q_weight,
        q_bias,
        k_weight,
        k_bias,
        v_weight,
        v_bias,
        o_weight,
        final_gain,
        *tables,
    )
    return hidden, embedding


def solution(mesh):
    in_specs = (
        P("seq", None),
        P(),
        P(),
        P(None, "head"),
        P("head"),
        P(None, "head"),
        P("head"),
        P(None, "head"),
        P("head"),
        P("head", None),
        P("head"),
    )
    out_specs = (P("seq", "head"), P("head"))
    step = functools.partial(body, mesh.shape["seq"], mesh.shape["head"])
    return jax.shard_map(step, mesh=mesh, in_specs=in_specs, out_specs=out_specs, check_vma=False)
```
